16 devices in a mesh: seqs: 2 (over y, z), states: 8 (over x, core).
Axes of the slice: x: 4, y: 2, z: 1, core: 2. Of those that a mesh axis runs over, the one named last changes fastest.
The devices are a block of a 4x4x8 slice.
Arguments:
- trans_mat: bfloat16 [16384, 16384], P(None, 'states')
- emit_mat: bfloat16 [16384, 10000], P('states')
- init_prob: float32 [16384], P('states')
- tokens: int32 [256, 32], P('seqs'), parts along dimension 0
Outputs:
- output 1: float32 [256, 32], P('seqs'), parts along dimension 0
- output 2: float32 [256, 16384], P('seqs', 'states'), parts along dimension 0
There are 2 independent parts. The reference program is written for one: setup_inputs(seed, part) draws one part's arguments, and reference() takes and returns one part's arrays. A program takes and returns all parts, laid end to end along the dimension named above; an argument that names none is the same for every part.
All inputs are finite; a program needn't handle non-finite values.
Results may differ from the reference program's by a relative error of at most 0.00272.
Values are sent between devices in bfloat16 or wider.
A program may use at most 768 MiB of HBM per device.

```python
import jax
import jax.numpy as jnp
from jax import lax

K = 16384
V = 10000
B = 128
T = 32
ROW_BLOCK = min(K, 256)


def setup_inputs(seed: int = 0, part: int = 0) -> dict:
    base_key = jax.random.key(seed)
    key_trans, key_emit, key_init = jax.random.split(base_key, 3)
    key_tokens = jax.random.fold_in(jax.random.key(seed + 1), part)

    def trans_rows(block_id):
        logits = 2.0 * jax.random.normal(jax.random.fold_in(key_trans, block_id), (ROW_BLOCK, K), jnp.float32)
        row_probs = jax.nn.softmax(logits, axis=-1)
        row_ids = block_id * ROW_BLOCK + jnp.arange(ROW_BLOCK)
        self_mask = (jnp.arange(K)[None, :] == row_ids[:, None]).astype(jnp.float32)
        return (0.7 * row_probs + 0.3 * self_mask).astype(jnp.bfloat16)

    def emit_rows(block_id):
        logits = 2.5 * jax.random.normal(jax.random.fold_in(key_emit, block_id), (ROW_BLOCK, V), jnp.float32)
        return jax.nn.softmax(logits, axis=-1).astype(jnp.bfloat16)

    block_ids = jnp.arange(K // ROW_BLOCK)
    trans_mat = lax.map(trans_rows, block_ids).reshape(K, K)
    emit_mat = lax.map(emit_rows, block_ids).reshape(K, V)
    init_prob = jax.nn.softmax(3.0 * jax.random.normal(key_init, (K,), jnp.float32))
    tokens = jax.random.randint(key_tokens, (B, T), 0, V, jnp.int32)
    return {"trans_mat": trans_mat, "emit_mat": emit_mat, "init_prob": init_prob, "tokens": tokens}


def reference(trans_mat, emit_mat, init_prob, tokens):
    k_total, vocab_size = emit_mat.shape
    first_h = init_prob[None, :] * jnp.take(emit_mat, tokens[:, 0], axis=1).T.astype(jnp.float32)
    row_total = jnp.sum(first_h, axis=-1)
    alpha_start = first_h * (k_total / row_total)[:, None]

    def advance(alpha_prev, step_tokens):
        mixed_u = jnp.dot(alpha_prev.astype(jnp.bfloat16), trans_mat, preferred_element_type=jnp.float32)
        raw_h = mixed_u * jnp.take(emit_mat, step_tokens, axis=1).T.astype(jnp.float32)
        norm_c = jnp.sum(raw_h, axis=-1) / k_total
        return raw_h / norm_c[:, None], jnp.log(norm_c * vocab_size)

    alpha_final, step_logs = lax.scan(advance, alpha_start, tokens.T[1:])
    step_loglik = jnp.concatenate([jnp.log(row_total * vocab_size)[:, None], step_logs.T], axis=1)
    return step_loglik, alpha_final
```

```python
import functools

import jax
import jax.numpy as jnp
from jax import lax
from jax.experimental import pallas as pl
from jax.experimental.pallas import tpu as pltpu
from jax.sharding import PartitionSpec as P

MESH = pl.DeviceIdType.MESH
F32 = jnp.float32
BF16 = jnp.bfloat16
LANES = 128
SLOTS = 6
TILE = 256


def _when(cond, fn):
    if cond is True:
        fn()
    else:
        pl.when(cond)(fn)


def _forward_kernel(
    dims, a_hbm, e_hbm, pi_ref, tot_ref, out_ref,
    ad, ap, sb, go, gl, gd, gp, eb, cb, accv,
    a_sem, sb_sem, e_sem, own_s, pl_s, pl_r, d_r, f_s, dp_s, dp_r, c_s, c_r,
):
    n, steps, hb, kl = dims
    ck = kl // 4
    nx = n // 2
    k_total = n * kl
    ntiles = kl // TILE

    def run():
        me = lax.axis_index("states")
        x, core = me // 2, me % 2
        partner = 2 * x + 1 - core
        xr, xl, xf = (x + 1) % nx, (x + nx - 1) % nx, (x + 2) % nx
        right, left = 2 * xr + core, 2 * xl + core

        def remote(src, dst, ss, rs, dev):
            return pltpu.make_async_remote_copy(
                src_ref=src, dst_ref=dst, send_sem=ss, recv_sem=rs,
                device_id={"states": dev}, device_id_type=MESH,
            )

        def mm(half, parts):
            for nt in range(ntiles):
                cols = pl.ds(nt * TILE, TILE)
                total = accv[half, :, cols]
                for lhs, rhs in parts:
                    for q in range(rhs.shape[0]):
                        total += jnp.dot(lhs[q], rhs[q, :, cols], preferred_element_type=F32)
                accv[half, :, cols] = total

        def mm_joint(old, lhs, rhs, shared):
            for nt in range(ntiles):
                cols = pl.ds(nt * TILE, TILE)
                both = jnp.concatenate([accv[0, :, cols], accv[1, :, cols]], axis=0)
                for q in range(4):
                    rows = jnp.concatenate([shared[0, q], shared[1, q]], axis=0)
                    both += jnp.dot(rows, sb[q, :, cols], preferred_element_type=F32)
                own = both[old * hb : (old + 1) * hb]
                for q in range(rhs.shape[0]):
                    own += jnp.dot(lhs[q], rhs[q, :, cols], preferred_element_type=F32)
                accv[old, :, cols] = own
                accv[1 - old, :, cols] = both[(1 - old) * hb : (2 - old) * hb]

        def pop(half, nt):
            cols = pl.ds(nt * TILE, TILE)
            got = accv[half, :, cols]
            accv[half, :, cols] = jnp.zeros_like(got)
            return got

        def shard_rows(dev, q):
            return pl.ds(pl.multiple_of((dev * 4 + q) * ck, ck), ck)

        def sb_load(dev):
            return [
                pltpu.make_async_copy(a_hbm.at[shard_rows(dev, q)], sb.at[q], sb_sem.at[q])
                for q in range(4)
            ]

        def a_load(side, i):
            c = core if side == 0 else 1 - core
            dst = ad if side == 0 else ap
            if i < 4:
                src = [(2 * xl + c, i), (2 * xr + c, (i + 2) % 4)]
            else:
                src = [(2 * xf + c, i - 4), (2 * xf + c, i - 2)]
            return [
                pltpu.make_async_copy(a_hbm.at[shard_rows(dev, q)], dst.at[i, d], a_sem.at[side, i, d])
                for d, (dev, q) in enumerate(src)
            ]

        def a_wait(side, i):
            dst = ad if side == 0 else ap
            for d in range(2):
                pltpu.make_async_copy(
                    a_hbm.at[pl.ds(0, ck)], dst.at[i, d], a_sem.at[side, i, d]
                ).wait()

        def e_load(half, t):
            return pltpu.make_async_copy(e_hbm.at[t, half], eb.at[half], e_sem.at[half])

        def own_right(half, i):
            return remote(go.at[half, i], gd.at[half, i, 0], own_s.at[half, i, 0], d_r.at[half, i, 0], right)

        def own_left(half, i):
            q = (i + 2) % 4
            return remote(go.at[half, q], gd.at[half, i, 1], own_s.at[half, i, 1], d_r.at[half, i, 1], left)

        def own_partner(half):
            return remote(go.at[half], gl.at[half], pl_s.at[half], pl_r.at[half], partner)

        def fwd_right(half, i):
            return remote(gd.at[half, i, 0], gd.at[half, i + 4, 0], f_s.at[half, i, 0], d_r.at[half, i + 4, 0], right)

        def fwd_left(half, i):
            return remote(gd.at[half, i, 1], gd.at[half, i + 4, 1], f_s.at[half, i, 1], d_r.at[half, i + 4, 1], left)

        def fwd_partner(half, i):
            return remote(gd.at[half, i], gp.at[half, i], dp_s.at[half, i], dp_r.at[half, i], partner)

        def direct_wait(half, i):
            for d in range(2):
                remote(gd.at[half, i, d], gd.at[half, i, d], own_s.at[half, 0, d], d_r.at[half, i, d], right).wait_recv()

        def c_copy(half, j):
            return remote(cb.at[half, me], cb.at[half, me], c_s.at[half, j], c_r.at[half, me], (me + j) % n)

        def send_early(half):
            for i in range(3):
                own_right(half, i).start()
                own_left(half, i).start()
                if i == 0:
                    own_partner(half).start()

        def send_late(half):
            own_right(half, 3).start()
            own_left(half, 3).start()

        def direct(half, i, ring, first):
            direct_wait(half, i)

            def onward():
                fwd_right(half, i).start()
                fwd_left(half, i).start()

            if ring is not False:
                _when(ring, onward)
            fwd_partner(half, i).start()
            if first is not None:
                pl.when(first)(lambda: a_wait(0, i))

        def passed(half, i, first):
            fwd_partner(half, i).wait_recv()
            if first is not None:
                pl.when(first)(lambda: a_wait(1, i))

        def arrive(half, lo, hi, ring, first):
            def body(i, carry):
                direct(half, i, ring(i), first)
                passed(half, i - 1, first)
                mm(half, [(gd.at[half, i], ad.at[i]), (gp.at[half, i - 1], ap.at[i - 1])])
                return carry

            lax.fori_loop(lo, hi, body, 0)

        def sends_done(half):
            for i in range(4):
                own_right(half, i).wait_send()
                own_left(half, i).wait_send()
            own_partner(half).wait_send()
            for i in range(2):
                fwd_right(half, i).wait_send()
                fwd_left(half, i).wait_send()
            for i in range(SLOTS):
                fwd_partner(half, i).wait_send()

        def epilogue(half, t, start):
            e_load(half, 0).wait()
            part = jnp.zeros((hb, LANES), F32)
            for nt in range(ntiles):
                cols = pl.ds(nt * TILE, TILE)
                u = pop(half, nt)
                if start is not None:
                    pi_rows = jnp.broadcast_to(pi_ref[:, cols], (hb, TILE))
                    u = pi_rows if start is True else jnp.where(start, pi_rows, u)
                h = u * eb[half, :, cols].astype(F32)
                out_ref[half, :, cols] = h
                part = part + (h[:, :LANES] + h[:, LANES:])
            turned = jnp.concatenate([part] * (LANES // hb), axis=0).T
            cb[half, me] = jnp.sum(turned, axis=0, keepdims=True)
            pl.when(t + 1 < steps)(lambda: e_load(half, t + 1).start())
            for j in range(1, n):
                c_copy(half, j).start()

        def scale(half, t):
            for j in range(1, n):
                src = (me + j) % n
                remote(cb.at[half, src], cb.at[half, src], c_s.at[half, j], c_r.at[half, src], src).wait_recv()
                c_copy(half, j).wait_send()
            total = cb[half, 0]
            for j in range(1, n):
                total = total + cb[half, j]
            tot_ref[half, pl.ds(t, 1), :] = total
            inv = jnp.broadcast_to(k_total / total, (LANES, LANES)).T[:hb]
            for q in range(4):
                for s in range(ck // LANES):
                    cols = pl.ds(q * ck + s * LANES, LANES)
                    go[half, q, :, pl.ds(s * LANES, LANES)] = (out_ref[half, :, cols] * inv).astype(BF16)

            @pl.when(t == steps - 1)
            def _():
                for s in range(kl // LANES):
                    cols = pl.ds(s * LANES, LANES)
                    out_ref[half, :, cols] = out_ref[half, :, cols] * inv

        def phase(cur, old, k, live, have):
            start = None if have is True else jnp.logical_not(have)
            t = k + 1 if have is True else k
            _when(live, lambda: send_early(cur))
            old_first = k == 0 if old == 0 else None
            cur_first = k == 0 if cur == 0 else None
            last = SLOTS - 1

            def rest():
                arrive(old, 3, SLOTS, lambda i: False, old_first)
                passed(old, last, None)

            _when(have, rest)
            if cur == 0:
                pl.when(k == 0)(lambda: a_wait(1, last))
            else:
                own_partner(0).wait_recv()
                own_partner(1).wait_recv()
            for q in range(4):
                pltpu.make_async_copy(a_hbm.at[pl.ds(0, ck)], sb.at[q], sb_sem.at[q]).wait()
            mm_joint(old, gp.at[old, last], ap.at[last], go if cur == 0 else gl)

            def refill():
                for copy in sb_load(partner if cur == 0 else me):
                    copy.start()

            _when(live, refill)
            _when(have, lambda: sends_done(old))
            epilogue(old, t, start)

            def arrivals():
                send_late(cur)
                direct(cur, 0, True, cur_first)
                mm(cur, [(gd.at[cur, 0], ad.at[0])])
                arrive(cur, 1, 3, lambda i: i < 2, cur_first)

            _when(live, arrivals)
            scale(old, t)

        barrier = pltpu.get_barrier_semaphore()
        for j in range(1, n):
            pl.semaphore_signal(barrier, inc=1, device_id={"states": (me + j) % n}, device_id_type=MESH)
        accv[...] = jnp.zeros_like(accv)
        go[1] = jnp.zeros_like(go[1])
        gp[1, SLOTS - 1] = jnp.zeros_like(gp[1, SLOTS - 1])
        e_load(0, 0).start()
        e_load(1, 0).start()
        for c in sb_load(me):
            c.start()
        order = [(1, 5), (0, 0), (0, 1), (1, 0), (0, 2), (1, 1), (0, 3), (1, 2), (0, 4), (1, 3), (0, 5), (1, 4)]
        for side, i in order:
            for c in a_load(side, i):
                c.start()
        pl.semaphore_wait(barrier, n - 1)
        epilogue(0, 0, True)
        scale(0, 0)

        def step(k, carry):
            phase(0, 1, k, k < steps - 1, k >= 1)
            pl.when(k < steps - 1)(lambda: phase(1, 0, k, True, True))
            return carry

        lax.fori_loop(0, steps, step, 0)

    run()


def _forward(trans_mat, emit_steps, init_prob, n):
    k_total, kl = trans_mat.shape
    steps, _, hb, _ = emit_steps.shape
    ck = kl // 4
    dma = pltpu.SemaphoreType.DMA
    vmem = pl.BlockSpec(memory_space=pltpu.VMEM)
    hbm = pl.BlockSpec(memory_space=pl.ANY)
    return pl.pallas_call(
        functools.partial(_forward_kernel, (n, steps, hb, kl)),
        out_shape=(
            jax.ShapeDtypeStruct((2, steps, LANES), F32),
            jax.ShapeDtypeStruct((2, hb, kl), F32),
        ),
        in_specs=[hbm, hbm, vmem],
        out_specs=(vmem, vmem),
        scratch_shapes=[
            pltpu.VMEM((SLOTS, 2, ck, kl), BF16),
            pltpu.VMEM((SLOTS, 2, ck, kl), BF16),
            pltpu.VMEM((4, ck, kl), BF16),
            pltpu.VMEM((2, 4, hb, ck), BF16),
            pltpu.VMEM((2, 4, hb, ck), BF16),
            pltpu.VMEM((2, SLOTS, 2, hb, ck), BF16),
            pltpu.VMEM((2, SLOTS, 2, hb, ck), BF16),
            pltpu.VMEM((2, hb, kl), BF16),
            pltpu.VMEM((2, n, 1, LANES), F32),
            pltpu.VMEM((2, hb, kl), F32),
            dma((2, SLOTS, 2)),
            dma((4,)),
            dma((2,)),
            dma((2, 4, 2)),
            dma((2,)),
            dma((2,)),
            dma((2, SLOTS, 2)),
            dma((2, 2, 2)),
            dma((2, SLOTS)),
            dma((2, SLOTS)),
            dma((2, n)),
            dma((2, n)),
        ],
        compiler_params=pltpu.CompilerParams(
            collective_id=0, has_side_effects=True, vmem_limit_bytes=67043328
        ),
        name="hmm_forward",
    )(trans_mat, emit_steps, init_prob[None, :])


def solution(mesh):
    n = mesh.shape["states"]

    def local_forward(trans_mat, emit_mat, init_prob, tokens):
        vocab_size = emit_mat.shape[1]
        batch, steps = tokens.shape
        hb = batch // 2
        kl = trans_mat.shape[1]
        emit_steps = jnp.transpose(jnp.take(emit_mat, tokens.T, axis=1, mode="clip"), (1, 2, 0))
        totals, alpha = _forward(trans_mat, emit_steps.reshape(steps, 2, hb, kl), init_prob, n)
        norm = jnp.concatenate([totals[0, :, :hb], totals[1, :, :hb]], axis=1)
        first = jnp.arange(steps)[:, None] == 0
        norm = jnp.where(first, norm, norm / (n * kl))
        return jnp.log(norm * vocab_size).T, alpha.reshape(batch, kl)

    return jax.shard_map(
        local_forward,
        mesh=mesh,
        in_specs=(P(None, "states"), P("states", None), P("states"), P("seqs", None)),
        out_specs=(P("seqs", None), P("seqs", "states")),
        check_vma=False,
    )
```

```python
import functools

import jax
import jax.numpy as jnp
from jax import lax
from jax.experimental import pallas as pl
from jax.experimental.pallas import tpu as pltpu
from jax.sharding import PartitionSpec as P

MESH = pl.DeviceIdType.MESH
F32 = jnp.float32
BF16 = jnp.bfloat16
LANES = 128
SLOTS = 6
TILE = 256


def _when(cond, fn):
    if cond is True:
        fn()
    else:
        pl.when(cond)(fn)


def _forward_kernel(
    dims, a_hbm, e_hbm, pi_ref, tot_ref, out_ref,
    ad, ap, sb, go, gl, gd, gp, eb, cb, accv,
    a_sem, sb_sem, e_sem, own_s, pl_s, pl_r, d_r, f_s, dp_s, dp_r, c_s, c_r,
):
    n, steps, hb, kl = dims
    ck = kl // 4
    nx = n // 2
    k_total = n * kl
    ntiles = kl // TILE

    def run():
        me = lax.axis_index("states")
        x, core = me // 2, me % 2
        partner = 2 * x + 1 - core
        xr, xl, xf = (x + 1) % nx, (x + nx - 1) % nx, (x + 2) % nx
        right, left = 2 * xr + core, 2 * xl + core

        def remote(src, dst, ss, rs, dev):
            return pltpu.make_async_remote_copy(
                src_ref=src, dst_ref=dst, send_sem=ss, recv_sem=rs,
                device_id={"states": dev}, device_id_type=MESH,
            )

        def mm(half, parts):
            for nt in range(ntiles):
                cols = pl.ds(nt * TILE, TILE)
                total = accv[half, :, cols]
                for lhs, rhs in parts:
                    for q in range(rhs.shape[0]):
                        total += jnp.dot(lhs[q], rhs[q, :, cols], preferred_element_type=F32)
                accv[half, :, cols] = total

        def mm_joint(old, lhs, rhs, shared):
            for nt in range(ntiles):
                cols = pl.ds(nt * TILE, TILE)
                both = jnp.concatenate([accv[0, :, cols], accv[1, :, cols]], axis=0)
                for q in range(4):
                    rows = jnp.concatenate([shared[0, q], shared[1, q]], axis=0)
                    both += jnp.dot(rows, sb[q, :, cols], preferred_element_type=F32)
                own = both[old * hb : (old + 1) * hb]
                for q in range(rhs.shape[0]):
                    own += jnp.dot(lhs[q], rhs[q, :, cols], preferred_element_type=F32)
                accv[old, :, cols] = own
                accv[1 - old, :, cols] = both[(1 - old) * hb : (2 - old) * hb]

        def pop(half, nt):
            cols = pl.ds(nt * TILE, TILE)
            got = accv[half, :, cols]
            accv[half, :, cols] = jnp.zeros_like(got)
            return got

        def shard_rows(dev, q):
            return pl.ds(pl.multiple_of((dev * 4 + q) * ck, ck), ck)

        def sb_load(dev):
            return [
                pltpu.make_async_copy(a_hbm.at[shard_rows(dev, q)], sb.at[q], sb_sem.at[q])
                for q in range(4)
            ]

        def a_load(side, i):
            c = core if side == 0 else 1 - core
            dst = ad if side == 0 else ap
            if i < 4:
                src = [(2 * xl + c, i), (2 * xr + c, (i + 2) % 4)]
            else:
                src = [(2 * xf + c, i - 4), (2 * xf + c, i - 2)]
            return [
                pltpu.make_async_copy(a_hbm.at[shard_rows(dev, q)], dst.at[i, d], a_sem.at[side, i, d])
                for d, (dev, q) in enumerate(src)
            ]

        def a_wait(side, i):
            dst = ad if side == 0 else ap
            for d in range(2):
                pltpu.make_async_copy(
                    a_hbm.at[pl.ds(0, ck)], dst.at[i, d], a_sem.at[side, i, d]
                ).wait()

        def e_load(half, t):
            return pltpu.make_async_copy(e_hbm.at[t, half], eb.at[half], e_sem.at[half])

        def own_right(half, i):
            return remote(go.at[half, i], gd.at[half, i, 0], own_s.at[half, i, 0], d_r.at[half, i, 0], right)

        def own_left(half, i):
            q = (i + 2) % 4
            return remote(go.at[half, q], gd.at[half, i, 1], own_s.at[half, i, 1], d_r.at[half, i, 1], left)

        def own_partner(half):
            return remote(go.at[half], gl.at[half], pl_s.at[half], pl_r.at[half], partner)

        def fwd_right(half, i):
            return remote(gd.at[half, i, 0], gd.at[half, i + 4, 0], f_s.at[half, i, 0], d_r.at[half, i + 4, 0], right)

        def fwd_left(half, i):
            return remote(gd.at[half, i, 1], gd.at[half, i + 4, 1], f_s.at[half, i, 1], d_r.at[half, i + 4, 1], left)

        def fwd_partner(half, i):
            return remote(gd.at[half, i], gp.at[half, i], dp_s.at[half, i], dp_r.at[half, i], partner)

        def direct_wait(half, i):
            for d in range(2):
                remote(gd.at[half, i, d], gd.at[half, i, d], own_s.at[half, 0, d], d_r.at[half, i, d], right).wait_recv()

        def c_copy(half, j):
            return remote(cb.at[half, me], cb.at[half, me], c_s.at[half, j], c_r.at[half, me], (me + j) % n)

        def send_own(half):
            for i in range(4):
                own_right(half, i).start()
                own_left(half, i).start()
                if i == 0:
                    own_partner(half).start()

        def direct(half, i, ring, first):
            direct_wait(half, i)

            def onward():
                fwd_right(half, i).start()
                fwd_left(half, i).start()

            if ring is not False:
                _when(ring, onward)
            fwd_partner(half, i).start()
            if first is not None:
                pl.when(first)(lambda: a_wait(0, i))

        def passed(half, i, first):
            fwd_partner(half, i).wait_recv()
            if first is not None:
                pl.when(first)(lambda: a_wait(1, i))

        def arrive(half, lo, hi, ring, first, also=lambda i: None):
            def body(i, carry):
                direct(half, i, ring(i), first)
                also(i)
                passed(half, i - 1, first)
                mm(half, [(gd.at[half, i], ad.at[i]), (gp.at[half, i - 1], ap.at[i - 1])])
                return carry

            lax.fori_loop(lo, hi, body, 0)

        def sends_done(half):
            for i in range(4):
                own_right(half, i).wait_send()
                own_left(half, i).wait_send()
            own_partner(half).wait_send()
            for i in range(2):
                fwd_right(half, i).wait_send()
                fwd_left(half, i).wait_send()
            for i in range(SLOTS):
                fwd_partner(half, i).wait_send()

        def epilogue(half, t, start):
            e_load(half, 0).wait()
            part = jnp.zeros((hb, LANES), F32)
            for nt in range(ntiles):
                cols = pl.ds(nt * TILE, TILE)
                u = pop(half, nt)
                if start is not None:
                    pi_rows = jnp.broadcast_to(pi_ref[:, cols], (hb, TILE))
                    u = pi_rows if start is True else jnp.where(start, pi_rows, u)
                h = u * eb[half, :, cols].astype(F32)
                out_ref[half, :, cols] = h
                part = part + (h[:, :LANES] + h[:, LANES:])
            turned = jnp.concatenate([part] * (LANES // hb), axis=0).T
            cb[half, me] = jnp.sum(turned, axis=0, keepdims=True)
            for j in range(1, n):
                c_copy(half, j).start()
            pl.when(t + 1 < steps)(lambda: e_load(half, t + 1).start())

        def scale(half, t):
            for j in range(1, n):
                src = (me + j) % n
                remote(cb.at[half, src], cb.at[half, src], c_s.at[half, j], c_r.at[half, src], src).wait_recv()
                c_copy(half, j).wait_send()
            total = cb[half, 0]
            for j in range(1, n):
                total = total + cb[half, j]
            tot_ref[half, pl.ds(t, 1), :] = total
            inv = jnp.broadcast_to(k_total / total, (LANES, LANES)).T[:hb]
            for q in range(4):
                for s in range(ck // LANES):
                    cols = pl.ds(q * ck + s * LANES, LANES)
                    go[half, q, :, pl.ds(s * LANES, LANES)] = (out_ref[half, :, cols] * inv).astype(BF16)

            @pl.when(t == steps - 1)
            def _():
                for s in range(kl // LANES):
                    cols = pl.ds(s * LANES, LANES)
                    out_ref[half, :, cols] = out_ref[half, :, cols] * inv

        def phase(cur, old, k, live, have):
            start = None if have is True else jnp.logical_not(have)
            t = k + 1 if have is True else k
            _when(live, lambda: send_own(cur))
            old_first = k == 0 if old == 0 else None
            cur_first = k == 0 if cur == 0 else None
            last = SLOTS - 1

            def rest():
                arrive(old, 3, SLOTS, lambda i: False, old_first)
                passed(old, last, None)

            _when(have, rest)
            if cur == 0:
                pl.when(k == 0)(lambda: a_wait(1, last))
            else:
                own_partner(0).wait_recv()
                own_partner(1).wait_recv()
            for q in range(4):
                pltpu.make_async_copy(a_hbm.at[pl.ds(0, ck)], sb.at[q], sb_sem.at[q]).wait()
            mm_joint(old, gp.at[old, last], ap.at[last], go if cur == 0 else gl)

            def refill(i):
                copies = sb_load(partner if cur == 0 else me)
                for part in range(2):

                    @pl.when(i == part + 1)
                    def _():
                        copies[2 * part].start()
                        copies[2 * part + 1].start()

            _when(have, lambda: sends_done(old))
            epilogue(old, t, start)

            def arrivals():
                direct(cur, 0, True, cur_first)
                mm(cur, [(gd.at[cur, 0], ad.at[0])])
                arrive(cur, 1, 3, lambda i: i < 2, cur_first, refill)

            _when(live, arrivals)
            scale(old, t)

        barrier = pltpu.get_barrier_semaphore()
        for j in range(1, n):
            pl.semaphore_signal(barrier, inc=1, device_id={"states": (me + j) % n}, device_id_type=MESH)
        accv[...] = jnp.zeros_like(accv)
        go[1] = jnp.zeros_like(go[1])
        gp[1, SLOTS - 1] = jnp.zeros_like(gp[1, SLOTS - 1])
        e_load(0, 0).start()
        e_load(1, 0).start()
        for c in sb_load(me):
            c.start()
        order = [(1, 5), (0, 0), (0, 1), (1, 0), (0, 2), (1, 1), (0, 3), (1, 2), (0, 4), (1, 3), (0, 5), (1, 4)]
        for side, i in order:
            for c in a_load(side, i):
                c.start()
        pl.semaphore_wait(barrier, n - 1)
        epilogue(0, 0, True)
        scale(0, 0)

        def step(k, carry):
            phase(0, 1, k, k < steps - 1, k >= 1)
            pl.when(k < steps - 1)(lambda: phase(1, 0, k, True, True))
            return carry

        lax.fori_loop(0, steps, step, 0)

    run()


def _forward(trans_mat, emit_steps, init_prob, n):
    k_total, kl = trans_mat.shape
    steps, _, hb, _ = emit_steps.shape
    ck = kl // 4
    dma = pltpu.SemaphoreType.DMA
    vmem = pl.BlockSpec(memory_space=pltpu.VMEM)
    hbm = pl.BlockSpec(memory_space=pl.ANY)
    return pl.pallas_call(
        functools.partial(_forward_kernel, (n, steps, hb, kl)),
        out_shape=(
            jax.ShapeDtypeStruct((2, steps, LANES), F32),
            jax.ShapeDtypeStruct((2, hb, kl), F32),
        ),
        in_specs=[hbm, hbm, vmem],
        out_specs=(vmem, vmem),
        scratch_shapes=[
            pltpu.VMEM((SLOTS, 2, ck, kl), BF16),
            pltpu.VMEM((SLOTS, 2, ck, kl), BF16),
            pltpu.VMEM((4, ck, kl), BF16),
            pltpu.VMEM((2, 4, hb, ck), BF16),
            pltpu.VMEM((2, 4, hb, ck), BF16),
            pltpu.VMEM((2, SLOTS, 2, hb, ck), BF16),
            pltpu.VMEM((2, SLOTS, 2, hb, ck), BF16),
            pltpu.VMEM((2, hb, kl), BF16),
            pltpu.VMEM((2, n, 1, LANES), F32),
            pltpu.VMEM((2, hb, kl), F32),
            dma((2, SLOTS, 2)),
            dma((4,)),
            dma((2,)),
            dma((2, 4, 2)),
            dma((2,)),
            dma((2,)),
            dma((2, SLOTS, 2)),
            dma((2, 2, 2)),
            dma((2, SLOTS)),
            dma((2, SLOTS)),
            dma((2, n)),
            dma((2, n)),
        ],
        compiler_params=pltpu.CompilerParams(
            collective_id=0, has_side_effects=True, vmem_limit_bytes=67043328
        ),
        name="hmm_forward",
    )(trans_mat, emit_steps, init_prob[None, :])


def solution(mesh):
    n = mesh.shape["states"]

    def local_forward(trans_mat, emit_mat, init_prob, tokens):
        vocab_size = emit_mat.shape[1]
        batch, steps = tokens.shape
        hb = batch // 2
        kl = trans_mat.shape[1]
        emit_steps = jnp.transpose(jnp.take(emit_mat, tokens.T, axis=1, mode="clip"), (1, 2, 0))
        totals, alpha = _forward(trans_mat, emit_steps.reshape(steps, 2, hb, kl), init_prob, n)
        norm = jnp.concatenate([totals[0, :, :hb], totals[1, :, :hb]], axis=1)
        first = jnp.arange(steps)[:, None] == 0
        norm = jnp.where(first, norm, norm / (n * kl))
        return jnp.log(norm * vocab_size).T, alpha.reshape(batch, kl)

    return jax.shard_map(
        local_forward,
        mesh=mesh,
        in_specs=(P(None, "states"), P("states", None), P("states"), P("seqs", None)),
        out_specs=(P("seqs", None), P("seqs", "states")),
        check_vma=False,
    )
```

```python
import functools

import jax
import jax.numpy as jnp
from jax import lax
from jax.experimental import pallas as pl
from jax.experimental.pallas import tpu as pltpu
from jax.sharding import PartitionSpec as P

MESH = pl.DeviceIdType.MESH
F32 = jnp.float32
BF16 = jnp.bfloat16
LANES = 128
BUFS = 4
SLOTS = 6
TILE = 256


def _when(cond, fn):
    if cond is True:
        fn()
    else:
        pl.when(cond)(fn)


def _forward_kernel(
    dims, a_hbm, e_hbm, pi_ref, tot_ref, out_ref,
    ad, ap, sb, go, gd, gp, eb, cb, accv,
    a_sem, sb_sem, e_sem, own_s, pl_s, pl_r, d_r, f_s, dp_s, dp_r, c_s, c_r,
):
    n, steps, hb, kl = dims
    ck = kl // 4
    nx = n // 2
    k_total = n * kl
    ntiles = kl // TILE

    def run():
        me = lax.axis_index("states")
        x, core = me // 2, me % 2
        partner = 2 * x + 1 - core
        xr, xl, xf = (x + 1) % nx, (x + nx - 1) % nx, (x + 2) % nx
        right, left = 2 * xr + core, 2 * xl + core

        def remote(src, dst, ss, rs, dev):
            return pltpu.make_async_remote_copy(
                src_ref=src, dst_ref=dst, send_sem=ss, recv_sem=rs,
                device_id={"states": dev}, device_id_type=MESH,
            )

        def mm(half, parts):
            for nt in range(ntiles):
                cols = pl.ds(nt * TILE, TILE)
                total = accv[half, :, cols]
                for lhs, rhs in parts:
                    for q in range(rhs.shape[0]):
                        total += jnp.dot(lhs[q], rhs[q, :, cols], preferred_element_type=F32)
                accv[half, :, cols] = total

        def mm_joint(cur, old, lhs, rhs, shared):
            for nt in range(ntiles):
                cols = pl.ds(nt * TILE, TILE)
                both = jnp.concatenate([accv[cur, :, cols], accv[old, :, cols]], axis=0)
                for q in range(4):
                    rows = jnp.concatenate([shared[cur, q], shared[old, q]], axis=0)
                    both += jnp.dot(rows, sb[q, :, cols], preferred_element_type=F32)
                own = both[hb:]
                for q in range(rhs.shape[0]):
                    own += jnp.dot(lhs[q], rhs[q, :, cols], preferred_element_type=F32)
                accv[old, :, cols] = own
                accv[cur, :, cols] = both[:hb]

        def pop(half, nt):
            cols = pl.ds(nt * TILE, TILE)
            got = accv[half, :, cols]
            accv[half, :, cols] = jnp.zeros_like(got)
            return got

        def shard_rows(dev, q):
            return pl.ds(pl.multiple_of((dev * 4 + q) * ck, ck), ck)

        def sb_load(dev):
            return [
                pltpu.make_async_copy(a_hbm.at[shard_rows(dev, q)], sb.at[q], sb_sem.at[q])
                for q in range(4)
            ]

        def a_load(side, i):
            c = core if side == 0 else 1 - core
            dst = ad if side == 0 else ap
            if i < 4:
                src = [(2 * xl + c, i), (2 * xr + c, (i + 2) % 4)]
            else:
                src = [(2 * xf + c, i - 4), (2 * xf + c, i - 2)]
            return [
                pltpu.make_async_copy(a_hbm.at[shard_rows(dev, q)], dst.at[i, d], a_sem.at[side, i, d])
                for d, (dev, q) in enumerate(src)
            ]

        def a_wait(side, i):
            dst = ad if side == 0 else ap
            for d in range(2):
                pltpu.make_async_copy(
                    a_hbm.at[pl.ds(0, ck)], dst.at[i, d], a_sem.at[side, i, d]
                ).wait()

        def e_load(half, t):
            return pltpu.make_async_copy(e_hbm.at[t, half], eb.at[half], e_sem.at[half])

        def own_right(half, i):
            return remote(go.at[0, half, i], gd.at[half, i, 0], own_s.at[half, i, 0], d_r.at[half, i, 0], right)

        def own_left(half, i):
            q = (i + 2) % 4
            return remote(go.at[0, half, q], gd.at[half, i, 1], own_s.at[half, i, 1], d_r.at[half, i, 1], left)

        def own_partner(half):
            return remote(go.at[0, half], go.at[1, half], pl_s.at[half], pl_r.at[half], partner)

        def fwd_right(half, i):
            return remote(gd.at[half, i, 0], gd.at[half, i + 4, 0], f_s.at[half, i, 0], d_r.at[half, i + 4, 0], right)

        def fwd_left(half, i):
            return remote(gd.at[half, i, 1], gd.at[half, i + 4, 1], f_s.at[half, i, 1], d_r.at[half, i + 4, 1], left)

        def fwd_partner(half, i):
            return remote(gd.at[half, i], gp.at[half, i], dp_s.at[half, i], dp_r.at[half, i], partner)

        def direct_wait(half, i):
            for d in range(2):
                remote(gd.at[half, i, d], gd.at[half, i, d], own_s.at[half, 0, d], d_r.at[half, i, d], right).wait_recv()

        def c_copy(half, j):
            return remote(cb.at[half, me], cb.at[half, me], c_s.at[half, j], c_r.at[half, me], (me + j) % n)

        def send_own(half):
            for i in range(4):
                own_right(half, i).start()
                own_left(half, i).start()
                if i == 0:
                    own_partner(half).start()

        def direct(half, i, ring, first):
            direct_wait(half, i)

            def onward():
                fwd_right(half, i).start()
                fwd_left(half, i).start()

            if ring is not False:
                _when(ring, onward)
            fwd_partner(half, i).start()
            if first is not None:
                pl.when(first)(lambda: a_wait(0, i))

        def passed(half, i, first):
            fwd_partner(half, i).wait_recv()
            if first is not None:
                pl.when(first)(lambda: a_wait(1, i))

        def arrive(half, lo, hi, ring, first, also=lambda i: None):
            def body(i, carry):
                direct(half, i, ring(i), first)
                also(i)
                passed(half, i - 1, first)
                mm(half, [(gd.at[half, i], ad.at[i]), (gp.at[half, i - 1], ap.at[i - 1])])
                return carry

            lax.fori_loop(lo, hi, body, 0)

        def sends_done(half):
            for i in range(4):
                own_right(half, i).wait_send()
                own_left(half, i).wait_send()
            own_partner(half).wait_send()
            for i in range(2):
                fwd_right(half, i).wait_send()
                fwd_left(half, i).wait_send()
            for i in range(SLOTS):
                fwd_partner(half, i).wait_send()

        def epilogue(half, t, start):
            e_load(half, 0).wait()
            part = jnp.zeros((hb, LANES), F32)
            for nt in range(ntiles):
                cols = pl.ds(nt * TILE, TILE)
                u = pop(half, nt)
                if start is not None:
                    pi_rows = jnp.broadcast_to(pi_ref[:, cols], (hb, TILE))
                    u = pi_rows if start is True else jnp.where(start, pi_rows, u)
                h = u * eb[half, :, cols].astype(F32)
                out_ref[half, :, cols] = h
                part = part + (h[:, :LANES] + h[:, LANES:])
            turned = jnp.concatenate([part] * (LANES // hb), axis=0).T
            cb[half, me] = jnp.sum(turned, axis=0, keepdims=True)
            for j in range(1, n):
                c_copy(half, j).start()
            pl.when(t + 1 < steps)(lambda: e_load(half, t + 1).start())

        def scale(half, t):
            for j in range(1, n):
                src = (me + j) % n
                remote(cb.at[half, src], cb.at[half, src], c_s.at[half, j], c_r.at[half, src], src).wait_recv()
                c_copy(half, j).wait_send()
            total = cb[half, 0]
            for j in range(1, n):
                total = total + cb[half, j]
            tot_ref[half, pl.ds(t, 1), :] = total
            inv = jnp.broadcast_to(k_total / total, (LANES, LANES)).T[:hb]
            for q in range(4):
                for s in range(ck // LANES):
                    cols = pl.ds(q * ck + s * LANES, LANES)
                    go[0, half, q, :, pl.ds(s * LANES, LANES)] = (out_ref[half, :, cols] * inv).astype(BF16)

            @pl.when(t == steps - 1)
            def _():
                for s in range(kl // LANES):
                    cols = pl.ds(s * LANES, LANES)
                    out_ref[half, :, cols] = out_ref[half, :, cols] * inv

        def phase(p, carry):
            cur = lax.rem(p, 2)
            old = 1 - cur
            t = lax.div(p + 1, 2)
            last = SLOTS - 1
            live = p < 2 * steps - 2
            have = p >= 1
            pl.when(live)(lambda: send_own(cur))

            @pl.when(have)
            def _():
                arrive(old, 3, SLOTS, lambda i: False, p == 1)
                passed(old, last, None)

            pl.when(p == 0)(lambda: a_wait(1, last))

            @pl.when(cur == 1)
            def _():
                own_partner(0).wait_recv()
                own_partner(1).wait_recv()

            for q in range(4):
                pltpu.make_async_copy(a_hbm.at[pl.ds(0, ck)], sb.at[q], sb_sem.at[q]).wait()
            mm_joint(cur, old, gp.at[old, last], ap.at[last], go.at[cur])
            pl.when(have)(lambda: sends_done(old))
            epilogue(old, t, p == 0)
            following = partner * (1 - cur) + me * cur

            def refill(i):
                copies = sb_load(following)
                for part in range(2):

                    @pl.when(i == part + 1)
                    def _():
                        copies[2 * part].start()
                        copies[2 * part + 1].start()

            @pl.when(live)
            def _():
                direct(cur, 0, True, p == 0)
                mm(cur, [(gd.at[cur, 0], ad.at[0])])
                arrive(cur, 1, 3, lambda i: i < 2, p == 0, refill)

            scale(old, t)
            return carry

        barrier = pltpu.get_barrier_semaphore()
        for j in range(1, n):
            pl.semaphore_signal(barrier, inc=1, device_id={"states": (me + j) % n}, device_id_type=MESH)
        accv[...] = jnp.zeros_like(accv)
        go[0, 1] = jnp.zeros_like(go[0, 1])
        gp[1, SLOTS - 1] = jnp.zeros_like(gp[1, SLOTS - 1])
        e_load(0, 0).start()
        e_load(1, 0).start()
        for c in sb_load(me):
            c.start()
        order = [(1, 5), (0, 0), (0, 1), (1, 0), (0, 2), (1, 1), (0, 3), (1, 2), (0, 4), (1, 3), (0, 5), (1, 4)]
        for side, i in order:
            for c in a_load(side, i):
                c.start()
        pl.semaphore_wait(barrier, n - 1)
        epilogue(0, 0, True)
        scale(0, 0)

        lax.fori_loop(0, 2 * steps - 1, phase, 0)

    run()


def _forward(trans_mat, emit_steps, init_prob, n):
    k_total, kl = trans_mat.shape
    steps, _, hb, _ = emit_steps.shape
    ck = kl // 4
    dma = pltpu.SemaphoreType.DMA
    vmem = pl.BlockSpec(memory_space=pltpu.VMEM)
    hbm = pl.BlockSpec(memory_space=pl.ANY)
    return pl.pallas_call(
        functools.partial(_forward_kernel, (n, steps, hb, kl)),
        out_shape=(
            jax.ShapeDtypeStruct((2, steps, LANES), F32),
            jax.ShapeDtypeStruct((2, hb, kl), F32),
        ),
        in_specs=[hbm, hbm, vmem],
        out_specs=(vmem, vmem),
        scratch_shapes=[
            pltpu.VMEM((SLOTS, 2, ck, kl), BF16),
            pltpu.VMEM((SLOTS, 2, ck, kl), BF16),
            pltpu.VMEM((4, ck, kl), BF16),
            pltpu.VMEM((2, 2, 4, hb, ck), BF16),
            pltpu.VMEM((2, SLOTS, 2, hb, ck), BF16),
            pltpu.VMEM((2, SLOTS, 2, hb, ck), BF16),
            pltpu.VMEM((2, hb, kl), BF16),
            pltpu.VMEM((2, n, 1, LANES), F32),
            pltpu.VMEM((2, hb, kl), F32),
            dma((2, SLOTS, 2)),
            dma((4,)),
            dma((2,)),
            dma((2, 4, 2)),
            dma((2,)),
            dma((2,)),
            dma((2, SLOTS, 2)),
            dma((2, 2, 2)),
            dma((2, SLOTS)),
            dma((2, SLOTS)),
            dma((2, n)),
            dma((2, n)),
        ],
        compiler_params=pltpu.CompilerParams(
            collective_id=0, has_side_effects=True, vmem_limit_bytes=67043328
        ),
        name="hmm_forward",
    )(trans_mat, emit_steps, init_prob[None, :])


def _gather_kernel(tok_ref, sub_ref, em_hbm, out_ref, buf, sem):
    g, groups = pl.program_id(0), pl.num_programs(0)
    hb = out_ref.shape[0]

    def fetch(group, slot):
        for b in range(hb):
            row = lax.shift_left(lax.shift_right_logical(tok_ref[group * hb + b], 3), 3)
            pltpu.make_async_copy(
                em_hbm.at[pl.ds(pl.multiple_of(row, 8), 8)], buf.at[slot, pl.ds(b * 8, 8)], sem.at[slot]
            ).start(priority=b % 2)

    slot = lax.rem(g, BUFS)

    @pl.when(g == 0)
    def _():
        for ahead in range(BUFS - 1):
            fetch(ahead, ahead)

    @pl.when(g + BUFS - 1 < groups)
    def _():
        fetch(g + BUFS - 1, lax.rem(g + BUFS - 1, BUFS))

    pltpu.make_async_copy(em_hbm.at[pl.ds(0, hb * 8)], buf.at[slot], sem.at[slot]).wait()
    col = lax.broadcasted_iota(jnp.int32, (hb, hb * 8), 1)
    row = lax.broadcasted_iota(jnp.int32, (hb, hb * 8), 0)
    pick = (col == row * 8 + sub_ref[...]).astype(F32).astype(BF16)
    out_ref[...] = jnp.dot(pick, buf[slot], preferred_element_type=F32).astype(BF16)


def _gather_rows(table, tokens, hb):
    kl = table.shape[1]
    count = tokens.shape[0]
    return pl.pallas_call(
        _gather_kernel,
        grid_spec=pltpu.PrefetchScalarGridSpec(
            num_scalar_prefetch=1,
            grid=(count // hb,),
            in_specs=[pl.BlockSpec((hb, 1), lambda g, t: (g, 0)), pl.BlockSpec(memory_space=pl.ANY)],
            out_specs=pl.BlockSpec((hb, kl), lambda g, t: (g, 0)),
            scratch_shapes=[pltpu.VMEM((BUFS, hb * 8, kl), BF16), pltpu.SemaphoreType.DMA((BUFS,))],
        ),
        out_shape=jax.ShapeDtypeStruct((count, kl), BF16),
        compiler_params=pltpu.CompilerParams(vmem_limit_bytes=67043328),
        name="emit_gather",
    )(tokens, lax.bitwise_and(tokens, 7)[:, None], table)


def solution(mesh):
    n = mesh.shape["states"]

    def local_forward(trans_mat, emit_mat, init_prob, tokens):
        vocab_size = emit_mat.shape[1]
        batch, steps = tokens.shape
        hb = batch // 2
        kl = trans_mat.shape[1]
        emit_steps = _gather_rows(emit_mat.T, tokens.T.reshape(-1), hb)
        totals, alpha = _forward(trans_mat, emit_steps.reshape(steps, 2, hb, kl), init_prob, n)
        norm = jnp.concatenate([totals[0, :, :hb], totals[1, :, :hb]], axis=1)
        first = jnp.arange(steps)[:, None] == 0
        norm = jnp.where(first, norm, norm / (n * kl))
        return jnp.log(norm * vocab_size).T, alpha.reshape(batch, kl)

    return jax.shard_map(
        local_forward,
        mesh=mesh,
        in_specs=(P(None, "states"), P("states", None), P("states"), P("seqs", None)),
        out_specs=(P("seqs", None), P("seqs", "states")),
        check_vma=False,
    )
```

```python
import functools

import jax
import jax.numpy as jnp
from jax import lax
from jax.experimental import pallas as pl
from jax.experimental.pallas import tpu as pltpu
from jax.sharding import PartitionSpec as P

MESH = pl.DeviceIdType.MESH
F32 = jnp.float32
BF16 = jnp.bfloat16
LANES = 128
BUFS = 4
SLOTS = 6
TILE = 256


def _when(cond, fn):
    if cond is True:
        fn()
    else:
        pl.when(cond)(fn)


def _forward_kernel(
    dims, a_hbm, e_hbm, pi_ref, tot_ref, out_ref,
    ad, ap, sb, go, gl, gd, gp, eb, cb, accv,
    a_sem, sb_sem, e_sem, own_s, pl_s, pl_r, d_r, f_s, dp_s, dp_r, c_s, c_r,
):
    n, steps, hb, kl = dims
    ck = kl // 4
    nx = n // 2
    k_total = n * kl
    ntiles = kl // TILE

    def run():
        me = lax.axis_index("states")
        x, core = me // 2, me % 2
        partner = 2 * x + 1 - core
        xr, xl, xf = (x + 1) % nx, (x + nx - 1) % nx, (x + 2) % nx
        right, left = 2 * xr + core, 2 * xl + core

        def remote(src, dst, ss, rs, dev):
            return pltpu.make_async_remote_copy(
                src_ref=src, dst_ref=dst, send_sem=ss, recv_sem=rs,
                device_id={"states": dev}, device_id_type=MESH,
            )

        def mm(half, parts):
            for nt in range(ntiles):
                cols = pl.ds(nt * TILE, TILE)
                total = accv[half, :, cols]
                for lhs, rhs in parts:
                    for q in range(rhs.shape[0]):
                        total += jnp.dot(lhs[q], rhs[q, :, cols], preferred_element_type=F32)
                accv[half, :, cols] = total

        def mm_joint(old, lhs, rhs, shared):
            for nt in range(ntiles):
                cols = pl.ds(nt * TILE, TILE)
                both = jnp.concatenate([accv[0, :, cols], accv[1, :, cols]], axis=0)
                for q in range(4):
                    rows = jnp.concatenate([shared[0, q], shared[1, q]], axis=0)
                    both += jnp.dot(rows, sb[q, :, cols], preferred_element_type=F32)
                own = both[old * hb : (old + 1) * hb]
                for q in range(rhs.shape[0]):
                    own += jnp.dot(lhs[q], rhs[q, :, cols], preferred_element_type=F32)
                accv[old, :, cols] = own
                accv[1 - old, :, cols] = both[(1 - old) * hb : (2 - old) * hb]

        def pop(half, nt):
            cols = pl.ds(nt * TILE, TILE)
            got = accv[half, :, cols]
            accv[half, :, cols] = jnp.zeros_like(got)
            return got

        def shard_rows(dev, q):
            return pl.ds(pl.multiple_of((dev * 4 + q) * ck, ck), ck)

        def sb_load(dev):
            return [
                pltpu.make_async_copy(a_hbm.at[shard_rows(dev, q)], sb.at[q], sb_sem.at[q])
                for q in range(4)
            ]

        def a_load(side, i):
            c = core if side == 0 else 1 - core
            dst = ad if side == 0 else ap
            if i < 4:
                src = [(2 * xl + c, i), (2 * xr + c, (i + 2) % 4)]
            else:
                src = [(2 * xf + c, i - 4), (2 * xf + c, i - 2)]
            return [
                pltpu.make_async_copy(a_hbm.at[shard_rows(dev, q)], dst.at[i, d], a_sem.at[side, i, d])
                for d, (dev, q) in enumerate(src)
            ]

        def a_wait(side, i):
            dst = ad if side == 0 else ap
            for d in range(2):
                pltpu.make_async_copy(
                    a_hbm.at[pl.ds(0, ck)], dst.at[i, d], a_sem.at[side, i, d]
                ).wait()

        def e_load(half, t):
            return pltpu.make_async_copy(e_hbm.at[t, half], eb.at[half], e_sem.at[half])

        def own_right(half, i):
            return remote(go.at[half, i], gd.at[half, i, 0], own_s.at[half, i, 0], d_r.at[half, i, 0], right)

        def own_left(half, i):
            q = (i + 2) % 4
            return remote(go.at[half, q], gd.at[half, i, 1], own_s.at[half, i, 1], d_r.at[half, i, 1], left)

        def own_partner(half):
            return remote(go.at[half], gl.at[half], pl_s.at[half], pl_r.at[half], partner)

        def fwd_right(half, i):
            return remote(gd.at[half, i, 0], gd.at[half, i + 4, 0], f_s.at[half, i, 0], d_r.at[half, i + 4, 0], right)

        def fwd_left(half, i):
            return remote(gd.at[half, i, 1], gd.at[half, i + 4, 1], f_s.at[half, i, 1], d_r.at[half, i + 4, 1], left)

        def fwd_partner(half, i):
            return remote(gd.at[half, i], gp.at[half, i], dp_s.at[half, i], dp_r.at[half, i], partner)

        def direct_wait(half, i):
            for d in range(2):
                remote(gd.at[half, i, d], gd.at[half, i, d], own_s.at[half, 0, d], d_r.at[half, i, d], right).wait_recv()

        def c_copy(half, j):
            return remote(cb.at[half, me], cb.at[half, me], c_s.at[half, j], c_r.at[half, me], (me + j) % n)

        def send_own(half):
            for i in range(4):
                own_right(half, i).start()
                own_left(half, i).start()
                if i == 0:
                    own_partner(half).start()

        def direct(half, i, ring, first):
            direct_wait(half, i)

            def onward():
                fwd_right(half, i).start()
                fwd_left(half, i).start()

            if ring is not False:
                _when(ring, onward)
            fwd_partner(half, i).start()
            if first is not None:
                pl.when(first)(lambda: a_wait(0, i))

        def passed(half, i, first):
            fwd_partner(half, i).wait_recv()
            if first is not None:
                pl.when(first)(lambda: a_wait(1, i))

        def arrive(half, lo, hi, ring, first, also=lambda i: None):
            def body(i, carry):
                direct(half, i, ring(i), first)
                also(i)
                passed(half, i - 1, first)
                mm(half, [(gd.at[half, i], ad.at[i]), (gp.at[half, i - 1], ap.at[i - 1])])
                return carry

            lax.fori_loop(lo, hi, body, 0)

        def sends_done(half):
            for i in range(4):
                own_right(half, i).wait_send()
                own_left(half, i).wait_send()
            own_partner(half).wait_send()
            for i in range(2):
                fwd_right(half, i).wait_send()
                fwd_left(half, i).wait_send()
            for i in range(SLOTS):
                fwd_partner(half, i).wait_send()

        def epilogue(half, t, start):
            e_load(half, 0).wait()
            part = jnp.zeros((hb, LANES), F32)
            for nt in range(ntiles):
                cols = pl.ds(nt * TILE, TILE)
                u = pop(half, nt)
                if start is not None:
                    pi_rows = jnp.broadcast_to(pi_ref[:, cols], (hb, TILE))
                    u = pi_rows if start is True else jnp.where(start, pi_rows, u)
                h = u * eb[half, :, cols].astype(F32)
                out_ref[half, :, cols] = h
                part = part + (h[:, :LANES] + h[:, LANES:])
            turned = jnp.concatenate([part] * (LANES // hb), axis=0).T
            cb[half, me] = jnp.sum(turned, axis=0, keepdims=True)
            for j in range(1, n):
                c_copy(half, j).start()
            pl.when(t + 1 < steps)(lambda: e_load(half, t + 1).start())

        def scale(half, t):
            for j in range(1, n):
                src = (me + j) % n
                remote(cb.at[half, src], cb.at[half, src], c_s.at[half, j], c_r.at[half, src], src).wait_recv()
                c_copy(half, j).wait_send()
            total = cb[half, 0]
            for j in range(1, n):
                total = total + cb[half, j]
            tot_ref[half, pl.ds(t, 1), :] = total
            inv = jnp.broadcast_to(k_total / total, (LANES, LANES)).T[:hb]
            for q in range(4):
                for s in range(ck // LANES):
                    cols = pl.ds(q * ck + s * LANES, LANES)
                    go[half, q, :, pl.ds(s * LANES, LANES)] = (out_ref[half, :, cols] * inv).astype(BF16)

            @pl.when(t == steps - 1)
            def _():
                for s in range(kl // LANES):
                    cols = pl.ds(s * LANES, LANES)
                    out_ref[half, :, cols] = out_ref[half, :, cols] * inv

        def phase(cur, old, k, live, have):
            start = None if have is True else jnp.logical_not(have)
            t = k + 1 if have is True else k
            _when(live, lambda: send_own(cur))
            old_first = k == 0 if old == 0 else None
            cur_first = k == 0 if cur == 0 else None
            last = SLOTS - 1

            def rest():
                arrive(old, 3, SLOTS, lambda i: False, old_first)
                passed(old, last, None)

            _when(have, rest)
            if cur == 0:
                pl.when(k == 0)(lambda: a_wait(1, last))
            else:
                own_partner(0).wait_recv()
                own_partner(1).wait_recv()
            for q in range(4):
                pltpu.make_async_copy(a_hbm.at[pl.ds(0, ck)], sb.at[q], sb_sem.at[q]).wait()
            mm_joint(old, gp.at[old, last], ap.at[last], go if cur == 0 else gl)

            def refill(i):
                copies = sb_load(partner if cur == 0 else me)
                for part in range(2):

                    @pl.when(i == part + 1)
                    def _():
                        copies[2 * part].start()
                        copies[2 * part + 1].start()

            _when(have, lambda: sends_done(old))
            epilogue(old, t, start)

            def arrivals():
                direct(cur, 0, True, cur_first)
                mm(cur, [(gd.at[cur, 0], ad.at[0])])
                arrive(cur, 1, 3, lambda i: i < 2, cur_first, refill)

            _when(live, arrivals)
            scale(old, t)

        barrier = pltpu.get_barrier_semaphore()
        for j in range(1, n):
            pl.semaphore_signal(barrier, inc=1, device_id={"states": (me + j) % n}, device_id_type=MESH)
        accv[...] = jnp.zeros_like(accv)
        go[1] = jnp.zeros_like(go[1])
        gp[1, SLOTS - 1] = jnp.zeros_like(gp[1, SLOTS - 1])
        e_load(0, 0).start()
        e_load(1, 0).start()
        for c in sb_load(me):
            c.start()
        order = [(1, 5), (0, 0), (0, 1), (1, 0), (0, 2), (1, 1), (0, 3), (1, 2), (0, 4), (1, 3), (0, 5), (1, 4)]
        for side, i in order:
            for c in a_load(side, i):
                c.start()
        pl.semaphore_wait(barrier, n - 1)
        epilogue(0, 0, True)
        scale(0, 0)

        def step(k, carry):
            phase(0, 1, k, k < steps - 1, k >= 1)
            pl.when(k < steps - 1)(lambda: phase(1, 0, k, True, True))
            return carry

        lax.fori_loop(0, steps, step, 0)

    run()


def _forward(trans_mat, emit_steps, init_prob, n):
    k_total, kl = trans_mat.shape
    steps, _, hb, _ = emit_steps.shape
    ck = kl // 4
    dma = pltpu.SemaphoreType.DMA
    vmem = pl.BlockSpec(memory_space=pltpu.VMEM)
    hbm = pl.BlockSpec(memory_space=pl.ANY)
    return pl.pallas_call(
        functools.partial(_forward_kernel, (n, steps, hb, kl)),
        out_shape=(
            jax.ShapeDtypeStruct((2, steps, LANES), F32),
            jax.ShapeDtypeStruct((2, hb, kl), F32),
        ),
        in_specs=[hbm, hbm, vmem],
        out_specs=(vmem, vmem),
        scratch_shapes=[
            pltpu.VMEM((SLOTS, 2, ck, kl), BF16),
            pltpu.VMEM((SLOTS, 2, ck, kl), BF16),
            pltpu.VMEM((4, ck, kl), BF16),
            pltpu.VMEM((2, 4, hb, ck), BF16),
            pltpu.VMEM((2, 4, hb, ck), BF16),
            pltpu.VMEM((2, SLOTS, 2, hb, ck), BF16),
            pltpu.VMEM((2, SLOTS, 2, hb, ck), BF16),
            pltpu.VMEM((2, hb, kl), BF16),
            pltpu.VMEM((2, n, 1, LANES), F32),
            pltpu.VMEM((2, hb, kl), F32),
            dma((2, SLOTS, 2)),
            dma((4,)),
            dma((2,)),
            dma((2, 4, 2)),
            dma((2,)),
            dma((2,)),
            dma((2, SLOTS, 2)),
            dma((2, 2, 2)),
            dma((2, SLOTS)),
            dma((2, SLOTS)),
            dma((2, n)),
            dma((2, n)),
        ],
        compiler_params=pltpu.CompilerParams(
            collective_id=0, has_side_effects=True, vmem_limit_bytes=67043328
        ),
        name="hmm_forward",
    )(trans_mat, emit_steps, init_prob[None, :])


def _gather_kernel(tok_ref, sub_ref, em_hbm, out_ref, buf, sem):
    g, groups = pl.program_id(0), pl.num_programs(0)
    hb = out_ref.shape[0]

    def fetch(group, slot):
        for b in range(hb):
            row = lax.shift_left(lax.shift_right_logical(tok_ref[group * hb + b], 3), 3)
            pltpu.make_async_copy(
                em_hbm.at[pl.ds(pl.multiple_of(row, 8), 8)], buf.at[slot, pl.ds(b * 8, 8)], sem.at[slot]
            ).start(priority=b % 2)

    slot = lax.rem(g, BUFS)

    @pl.when(g == 0)
    def _():
        for ahead in range(BUFS - 1):
            fetch(ahead, ahead)

    @pl.when(g + BUFS - 1 < groups)
    def _():
        fetch(g + BUFS - 1, lax.rem(g + BUFS - 1, BUFS))

    pltpu.make_async_copy(em_hbm.at[pl.ds(0, hb * 8)], buf.at[slot], sem.at[slot]).wait()
    col = lax.broadcasted_iota(jnp.int32, (hb, hb * 8), 1)
    row = lax.broadcasted_iota(jnp.int32, (hb, hb * 8), 0)
    pick = (col == row * 8 + sub_ref[...]).astype(F32).astype(BF16)
    out_ref[...] = jnp.dot(pick, buf[slot], preferred_element_type=F32).astype(BF16)


def _gather_rows(table, tokens, hb):
    kl = table.shape[1]
    count = tokens.shape[0]
    return pl.pallas_call(
        _gather_kernel,
        grid_spec=pltpu.PrefetchScalarGridSpec(
            num_scalar_prefetch=1,
            grid=(count // hb,),
            in_specs=[pl.BlockSpec((hb, 1), lambda g, t: (g, 0)), pl.BlockSpec(memory_space=pl.ANY)],
            out_specs=pl.BlockSpec((hb, kl), lambda g, t: (g, 0)),
            scratch_shapes=[pltpu.VMEM((BUFS, hb * 8, kl), BF16), pltpu.SemaphoreType.DMA((BUFS,))],
        ),
        out_shape=jax.ShapeDtypeStruct((count, kl), BF16),
        compiler_params=pltpu.CompilerParams(vmem_limit_bytes=67043328),
        name="emit_gather",
    )(tokens, lax.bitwise_and(tokens, 7)[:, None], table)


def solution(mesh):
    n = mesh.shape["states"]

    def local_forward(trans_mat, emit_mat, init_prob, tokens):
        vocab_size = emit_mat.shape[1]
        batch, steps = tokens.shape
        hb = batch // 2
        kl = trans_mat.shape[1]
        emit_steps = _gather_rows(emit_mat.T, tokens.T.reshape(-1), hb)
        totals, alpha = _forward(trans_mat, emit_steps.reshape(steps, 2, hb, kl), init_prob, n)
        norm = jnp.concatenate([totals[0, :, :hb], totals[1, :, :hb]], axis=1)
        first = jnp.arange(steps)[:, None] == 0
        norm = jnp.where(first, norm, norm / (n * kl))
        return jnp.log(norm * vocab_size).T, alpha.reshape(batch, kl)

    return jax.shard_map(
        local_forward,
        mesh=mesh,
        in_specs=(P(None, "states"), P("states", None), P("states"), P("seqs", None)),
        out_specs=(P("seqs", None), P("seqs", "states")),
        check_vma=False,
    )
```
